256 devices in a mesh: gx: 8 (over z), gy: 8 (over x, core), gz: 4 (over y).
Axes of the slice: x: 4, y: 4, z: 8, core: 2. Of those that a mesh axis runs over, the one named last changes fastest.
Arguments:
- displacement: float32 [3, 64, 256, 512], P(None, 'gx', 'gy', 'gz'), may hold values from -0.1 to 0.1
- velocity: float32 [3, 64, 256, 512], P(None, 'gx', 'gy', 'gz'), may hold values from -1.55 to 1.55
- energy: float32 [64, 256, 512], P('gx', 'gy', 'gz'), may hold values from 1 to 4
- density: float32 [64, 256, 512], P('gx', 'gy', 'gz'), may hold values from 0.5 to 4
- region: int32 [64, 256, 512], P('gx', 'gy', 'gz'), may hold values from 0 to 10
- adiabatic: float32 [11], replicated, may hold values from 1.2 to 1.8
- face_flags: int32 [6], replicated, may hold values from 0 to 1
Outputs:
- final_displacement: float32 [3, 64, 256, 512], P(None, 'gx', 'gy', 'gz')
- final_velocity: float32 [3, 64, 256, 512], P(None, 'gx', 'gy', 'gz')
- final_energy: float32 [64, 256, 512], P('gx', 'gy', 'gz')
The draws below stay inside these ranges and needn't reach their ends.
Inputs may be any that keep to these rules, and one draw needn't show every extreme that they name: `face_flags`: 1 marks a symmetry plane, 0 a free surface.
All inputs are finite; a program needn't handle non-finite values.
Results may differ from the reference program's by a relative error of at most 0.0003.
Values sent between devices are 32-bit elements; how exact they have to be, the bound alone decides.
No kernel may reach another device: no remote copies, remote signals or barrier semaphores. Data moves between devices by JAX's collectives and lax.ppermute only.
A program may use at most 64 MiB of HBM per device.

```python
import math
import jax
import jax.numpy as jnp
from jax import lax

STEPS = 2
REGIONS = 11
NX = 64
NY = 256
NZ = 512


def centred_ramp(extent, offset):
    places = (jnp.arange(extent, dtype=jnp.int32) + offset) % 6
    return places.astype(jnp.float32) - 2.5


def draw_velocity(key, part):
    phase_key = jax.random.fold_in(key, 11)
    noise_key = jax.random.fold_in(key, 12)
    phases = jax.random.randint(phase_key, (3,), 0, 6)
    ramp_slope = 0.25
    rough_part = jnp.clip(0.3 * jax.random.normal(noise_key, (3, NX, NY, NZ), jnp.float32), -0.9, 0.9)
    ramp_first = jnp.broadcast_to(centred_ramp(NX, phases[0])[:, None, None], (NX, NY, NZ))
    ramp_second = jnp.broadcast_to(centred_ramp(NY, phases[1])[None, :, None], (NX, NY, NZ))
    ramp_third = jnp.broadcast_to(centred_ramp(NZ, phases[2])[None, None, :], (NX, NY, NZ))
    converge = -ramp_slope * jnp.stack([ramp_first, ramp_second, ramp_third])
    return (converge + rough_part).astype(jnp.float32)


def touch_ends(values, key, smallest, top_value):
    index_at = [jax.random.randint(jax.random.fold_in(key, axis), (), 0, length) for axis, length in enumerate(values.shape)]
    widest = values.shape.index(max(values.shape))
    neighbour = index_at[:widest] + [(index_at[widest] + 1) % values.shape[widest]] + index_at[widest + 1:]
    return values.at[tuple(index_at)].set(smallest).at[tuple(neighbour)].set(top_value)


def steps_of(stream_key, shape, pieces, low, top_value):
    def one(axis_at, parts):
        draws = jax.random.uniform(jax.random.fold_in(jax.random.fold_in(stream_key, 6), axis_at), (parts,), jnp.float32, low / len(pieces), top_value / len(pieces))
        return jnp.repeat(jnp.exp(draws), shape[axis_at] // parts).reshape((-1,) + (1,) * (len(shape) - axis_at - 1))

    level = one(*pieces[0])
    for cut in pieces[1:]:
        level = level * one(*cut)
    return level


def normal_values(key, shape, scale, reach, split=(), kind=jnp.bfloat16):
    values = scale * jax.random.normal(key, shape, jnp.float32)
    if split:
        values = values * steps_of(key, shape, split, -0.22, 0.18)
    return jnp.clip(values, -reach, reach).astype(kind)


def setup_inputs(seed: int = 0) -> dict:
    seeds = jax.random.split(jax.random.key(seed), 8)
    displacement = normal_values(seeds[0], (3, NX, NY, NZ), 0.03, 0.1, ((1, 8), (2, 8), (3, 4)), jnp.float32)
    velocity = draw_velocity(jax.random.fold_in(seeds[7], 71), 0)
    energy = jnp.clip(jnp.exp(math.log(4.0) - 1.3862944 * jax.random.uniform(seeds[2], (NX, NY, NZ), jnp.float32) ** steps_of(seeds[2], (NX, NY, NZ), ((0, 8), (1, 8), (2, 4)), -0.2, 0.2)), 1.0, 4.0)
    density = jnp.clip(jnp.exp(math.log(4.0) - 2.0794415 * jax.random.uniform(seeds[3], (NX, NY, NZ), jnp.float32) ** steps_of(seeds[3], (NX, NY, NZ), ((0, 8), (1, 8), (2, 4)), -0.2, 0.2)), 0.5, 4.0)
    region = touch_ends(jax.random.randint(seeds[4], (NX, NY, NZ), 0, REGIONS), jax.random.fold_in(seeds[4], 1), 0, REGIONS - 1).astype(jnp.int32)
    adiabatic = jnp.clip(jax.random.uniform(seeds[5], (REGIONS,), jnp.float32, 1.2, 1.8), 1.2, 1.8)
    face_flags = touch_ends(jax.random.randint(seeds[6], (6,), 0, 2), jax.random.fold_in(seeds[6], 1), 0, 1).astype(jnp.int32)
    return dict(displacement=displacement, velocity=velocity, energy=energy, density=density, region=region, adiabatic=adiabatic, face_flags=face_flags)


COURANT = 0.25
QUAD_COEF = 1.0
LINEAR_COEF = 1.0
CORNERS = [(along_x, along_y, along_z) for along_x in (0, 1) for along_y in (0, 1) for along_z in (0, 1)]

def corner_views(extended, grid_shape):
    corner_sets = {}
    for offset in CORNERS:
        corner_sets[offset] = extended[:, offset[0]:offset[0] + grid_shape[0], offset[1]:offset[1] + grid_shape[1], offset[2]:offset[2] + grid_shape[2]]
    return corner_sets

def spread(corner_sets, start_comp):
    result = []
    for direction in range(3):
        accum = 0.0
        for offset in CORNERS:
            if offset[direction] == 1:
                accum = accum + corner_sets[offset][start_comp:start_comp + 3]
            else:
                accum = accum - corner_sets[offset][start_comp:start_comp + 3]
        result.append(0.25 * accum)
    return result

def cofactors(matrix):

    def minor_det(row_one, row_two, col_one, col_two):
        return matrix[row_one][col_one] * matrix[row_two][col_two] - matrix[row_one][col_two] * matrix[row_two][col_one]
    return [[minor_det(1, 2, 1, 2), -minor_det(1, 2, 0, 2), minor_det(1, 2, 0, 1)], [-minor_det(0, 2, 1, 2), minor_det(0, 2, 0, 2), -minor_det(0, 2, 0, 1)], [minor_det(0, 1, 1, 2), -minor_det(0, 1, 0, 2), minor_det(0, 1, 0, 1)]]

def kinematics(corner_sets):
    distorted = spread(corner_sets, 0)
    rate_terms = spread(corner_sets, 3)
    jacobian = [[distorted[direction][component] + (1.0 if component == direction else 0.0) for direction in range(3)] for component in range(3)]
    cofactor = cofactors(jacobian)
    volume = jacobian[0][0] * cofactor[0][0] + jacobian[0][1] * cofactor[0][1] + jacobian[0][2] * cofactor[0][2]
    change = 0.0
    for component in range(3):
        for direction in range(3):
            change = change + cofactor[component][direction] * rate_terms[direction][component]
    return (cofactor, volume, change / volume)

def minmod(forward, backward):
    return jnp.maximum(jnp.minimum(forward, backward), 0.0) + jnp.minimum(jnp.maximum(forward, backward), 0.0)

def face_ghosts(strain_rate, lower_rate, upper_rate, position, node_count, face_flags, dimension):
    lower_rate = jnp.where(position == 0, jnp.where(face_flags[2 * dimension] == 1, strain_rate, 0.0), lower_rate)
    upper_rate = jnp.where(position == node_count - 2, jnp.where(face_flags[2 * dimension + 1] == 1, strain_rate, 0.0), upper_rate)
    return (lower_rate, upper_rate)

def stress(strain_rate, roughness, volume, density, energy, gamma_elem, present):
    dense_now = density / volume
    length = jnp.cbrt(volume)
    compress = jnp.maximum(-strain_rate, 0.0)
    viscous = jnp.where(present, dense_now * length * length * compress * (QUAD_COEF * compress + LINEAR_COEF * roughness), 0.0)
    pressure = (gamma_elem - 1.0) * dense_now * energy
    sound_sq = gamma_elem * (gamma_elem - 1.0) * energy
    total_stress = jnp.where(present, pressure + viscous, 0.0)
    step_ratio = jnp.where(present, length / jnp.sqrt(sound_sq + viscous / dense_now), jnp.inf)
    return (total_stress, dense_now, step_ratio)

def corner_force(cofactor, total_stress, offset):
    corner_signs = [2.0 * corner_bit - 1.0 for corner_bit in offset]
    return jnp.stack([0.25 * total_stress * (corner_signs[0] * cofactor[component][0] + corner_signs[1] * cofactor[component][1] + corner_signs[2] * cofactor[component][2]) for component in range(3)])

def node_sum(term_of, grid_shape):
    accum = None
    for offset in CORNERS:
        corner_term = term_of(offset)
        padded = jnp.pad(corner_term, ((0, 0), (offset[0], 1 - offset[0]), (offset[1], 1 - offset[1]), (offset[2], 1 - offset[2])))
        accum = padded if accum is None else accum + padded
    return accum

def apply_walls(speeds, indices, counts, face_flags):
    components = []
    for dimension in range(3):
        on_wall = (indices[dimension] == 0) & (face_flags[2 * dimension] == 1) | (indices[dimension] == counts[dimension] - 1) & (face_flags[2 * dimension + 1] == 1)
        components.append(jnp.where(on_wall, 0.0, speeds[dimension]))
    return jnp.stack(components)

def reference(displacement, velocity, energy, density, region, adiabatic, face_flags):
    grid_shape = energy.shape
    indices = [jnp.arange(grid_shape[0], dtype=jnp.int32)[:, None, None], jnp.arange(grid_shape[1], dtype=jnp.int32)[None, :, None], jnp.arange(grid_shape[2], dtype=jnp.int32)[None, None, :]]
    present = (indices[0] < grid_shape[0] - 1) & (indices[1] < grid_shape[1] - 1) & (indices[2] < grid_shape[2] - 1)
    gamma_elem = adiabatic[region]
    mass_term = jnp.where(present, 0.125 * density, 0.0)[None]
    node_mass = node_sum(lambda offset: mass_term, grid_shape)[0, :grid_shape[0], :grid_shape[1], :grid_shape[2]]
    for step_index in range(STEPS):
        fields = jnp.concatenate([displacement, velocity], 0)
        extended = jnp.pad(fields, ((0, 0), (0, 1), (0, 1), (0, 1)))
        cofactor, volume, strain_rate = kinematics(corner_views(extended, grid_shape))
        roughness = 0.0
        for dimension in range(3):
            lower_pad = [(0, 0), (0, 0), (0, 0)]
            upper_pad = [(0, 0), (0, 0), (0, 0)]
            lower_pad[dimension] = (1, 0)
            upper_pad[dimension] = (0, 1)
            lower_rate = lax.slice_in_dim(jnp.pad(strain_rate, lower_pad), 0, grid_shape[dimension], axis=dimension)
            upper_rate = lax.slice_in_dim(jnp.pad(strain_rate, upper_pad), 1, grid_shape[dimension] + 1, axis=dimension)
            lower_rate, upper_rate = face_ghosts(strain_rate, lower_rate, upper_rate, indices[dimension], grid_shape[dimension], face_flags, dimension)
            roughness = roughness + jnp.abs(minmod(upper_rate - strain_rate, strain_rate - lower_rate))
        total_stress, dense_now, step_ratio = stress(strain_rate, roughness, volume, density, energy, gamma_elem, present)
        time_step = COURANT * jnp.min(step_ratio)
        force = node_sum(lambda offset: corner_force(cofactor, total_stress, offset), grid_shape)[:, :grid_shape[0], :grid_shape[1], :grid_shape[2]]
        velocity = apply_walls(velocity + time_step * force / node_mass, indices, grid_shape, face_flags)
        displacement = displacement + time_step * velocity
        energy = jnp.where(present, energy - time_step * total_stress * strain_rate / dense_now, energy)
    return (displacement, velocity, energy)
```

```python
import functools

import jax
import jax.numpy as jnp
from jax import lax
from jax.experimental import pallas as pl
from jax.experimental.pallas import tpu as pltpu
from jax.sharding import Mesh
from jax.sharding import PartitionSpec as P

GY = ("gy_0", "gy_1")
AXES = ("gx", "gy_0", "gy_1", "gz")

BX, BY, BZ = 8, 32, 128
PX = BX + 4
EX = BX + 1
ROWS = BY + 8
GROUPS = ROWS // 8
LANES = 2 * BZ
SLABS = 6 * PX + 3 * EX
PACKED = -(-SLABS * GROUPS // 32)
FAR = 1 << 20
MIB = 1 << 20


def next_z(v):
    return pltpu.roll(v, LANES - 1, 1)


def prev_z(v):
    return pltpu.roll(v, 1, 1)


def next_row(v):
    return pltpu.roll(v, 7, 0)


def prev_row(v):
    return pltpu.roll(v, 1, 0)


def slab_ids():
    for field in range(6):
        for plane in range(PX):
            yield field * PX + plane, field, plane
    for field in range(6, 9):
        for plane in range(EX):
            yield 6 * PX + (field - 6) * EX + plane, field, plane


def pack_x(gamma_table, disp, vel, energy, density, region, up, down, gamma):
    for field in range(6):
        src = disp if field < 3 else vel
        for p in range(2):
            up[2 * field + p] = src[field % 3, BX - 2 + p]
            down[2 * field + p] = src[field % 3, p]
    ids = region[...]
    value = jnp.zeros(ids.shape, jnp.float32)
    for r in range(gamma_table.shape[0]):
        value = jnp.where(ids == r, gamma_table[r], value)
    gamma[...] = value
    up[12] = energy[BX - 1]
    up[13] = density[BX - 1]
    up[14] = value[BX - 1]


def slab_source(field, plane, disp, vel, energy, density, gamma, x_low, x_high):
    if field < 6:
        if plane < 2:
            return x_low, (2 * field + plane,)
        if plane < BX + 2:
            return (disp if field < 3 else vel), (field % 3, plane - 2)
        return x_high, (2 * field + plane - BX - 2,)
    if plane == 0:
        return x_low, (12 + field - 6,)
    return (energy, density, gamma)[field - 6], (plane - 1,)


def pack_y(disp, vel, energy, density, gamma, x_low, x_high, up, down):
    for k, field, plane in slab_ids():
        ref, at = slab_source(field, plane, disp, vel, energy, density, gamma, x_low, x_high)
        up[4 * k : 4 * k + 4] = ref[(*at, slice(BY - 4, BY))]
        down[4 * k : 4 * k + 4] = ref[(*at, slice(0, 4))]


def pack_z(disp, vel, energy, density, gamma, x_low, x_high, y_low, y_high, main, up, down, stage):
    quad = lax.broadcasted_iota(jnp.int32, (8, BZ), 1) // 4
    for k, field, plane in slab_ids():
        ref, at = slab_source(field, plane, disp, vel, energy, density, gamma, x_low, x_high)
        stage[k, 0:4] = y_low[4 * k : 4 * k + 4]
        stage[k, 4 : BY + 4] = ref[(*at, slice(0, BY))]
        stage[k, BY + 4 : BY + 8] = y_high[4 * k : 4 * k + 4]
    for slot in range(PACKED):
        to_up = jnp.zeros((8, BZ), jnp.float32)
        to_down = jnp.zeros((8, BZ), jnp.float32)
        for q in range(32):
            n = 32 * slot + q
            if n >= SLABS * GROUPS:
                break
            k, j = divmod(n, GROUPS)
            value = stage[k, pl.ds(j, 8, stride=GROUPS), :]
            main[k, j] = value
            to_up = jnp.where(quad == q, pltpu.roll(value, (4 * q + 4) % BZ, 1), to_up)
            here = pltpu.roll(value, 4 * q, 1) if q else value
            to_down = jnp.where(quad == q, here, to_down)
        up[8 * slot : 8 * slot + 8] = to_up
        down[8 * slot : 8 * slot + 8] = to_down


class Place:
    def __init__(self, where):
        self.x0, self.y0, self.z0 = where[0], where[1], where[2]
        self.nx, self.ny, self.nz = where[3], where[4], where[5]
        self.flag = [where[6 + i] for i in range(6)]
        sublane = lax.broadcasted_iota(jnp.int32, (8, LANES), 0)
        lane = lax.broadcasted_iota(jnp.int32, (8, LANES), 1)
        self.row = GROUPS * sublane + (self.y0 - 4)
        self.col = jnp.where(lane < LANES - BZ // 2, lane, lane - LANES) + self.z0
        inside = (self.col >= 0) & (self.col < self.nz - 1)
        self.row_inside = jnp.where(inside, self.row, -FAR)

    def present(self, plane, j):
        x = self.x0 + plane
        ok = (x >= 0) & (x < self.nx - 1)
        top = jnp.where(ok, self.ny - 1 - j, -2 * FAR)
        return (self.row_inside >= -j) & (self.row_inside < top)

    def counted(self, plane, j):
        x = self.x0 + plane
        ok = (x >= 0) & (x < self.nx - 1)
        top = jnp.where(ok, jnp.minimum(self.ny - 1, self.y0 + BY) - j, -2 * FAR)
        rows = self.row_inside[:, :BZ]
        return (rows >= self.y0 - j) & (rows < top)


def open_factor(flag):
    return jnp.where(flag == 1, 0.0, 1.0)


def strain_pass(place, fs, fd, cof, vol, inv, strain):
    def plane_step(x, carry):
        for j in range(GROUPS):
            grad = []
            for f in range(6):
                a, b = fs[f, x, j], fs[f, x + 1, j]
                c, d = fs[f, x, j + 1], fs[f, x + 1, j + 1]
                p, q = d - a, b - c
                gz = (fd[f, x, j] + fd[f, x + 1, j]) + (fd[f, x, j + 1] + fd[f, x + 1, j + 1])
                grad.append([p + q, p - q, gz])
            m = [[grad[d][e] + 4.0 if d == e else grad[d][e] for e in range(3)] for d in range(3)]
            g = grad[3:]

            def minor(r, s, u, w):
                return m[r][u] * m[s][w] - m[r][w] * m[s][u]

            c = [
                [minor(1, 2, 1, 2), minor(1, 2, 2, 0), minor(1, 2, 0, 1)],
                [minor(2, 0, 1, 2), minor(2, 0, 2, 0), minor(2, 0, 0, 1)],
                [minor(0, 1, 1, 2), minor(0, 1, 2, 0), minor(0, 1, 0, 1)],
            ]
            volume = m[0][0] * c[0][0] + m[0][1] * c[0][1] + m[0][2] * c[0][2]
            change = c[0][0] * g[0][0]
            for d in range(3):
                for e in range(3):
                    if d or e:
                        change = change + c[d][e] * g[d][e]
                    cof[3 * d + e, x, j] = c[d][e]
            inverse = 1.0 / volume
            rate = change * inverse
            vol[x, j] = volume
            inv[x, j] = inverse
            strain[x, j + 1] = rate
            if j == 0:
                strain[x, GROUPS + 1] = next_row(rate)
            if j == GROUPS - 1:
                strain[x, 0] = prev_row(rate)
        return carry

    lax.fori_loop(0, PX - 1, plane_step, 0)


def limited(forward, backward):
    return jnp.maximum(jnp.minimum(forward, backward), 0.0) - jnp.minimum(
        jnp.maximum(forward, backward), 0.0
    )


def stress_pass(place, cof, vol, inv, strain, energy, density, gamma, terms, work, least):
    opened = [open_factor(f) for f in place.flag]

    def plane_step(i, low):
        x = i + 1
        gx = place.x0 + i - 1
        for j in range(GROUPS):
            s = strain[x, j + 1]
            back = jnp.where(gx == 0, s * opened[0], s - strain[x - 1, j + 1])
            fore = jnp.where(gx == place.nx - 2, -s * opened[1], strain[x + 1, j + 1] - s)
            rough = limited(fore, back)
            back = jnp.where(place.row == -j, s * opened[2], s - strain[x, j])
            fore = jnp.where(
                place.row == place.ny - 2 - j, -s * opened[3], strain[x, j + 2] - s
            )
            rough = rough + limited(fore, back)
            back = jnp.where(place.col == 0, s * opened[4], s - prev_z(s))
            fore = jnp.where(place.col == place.nz - 2, -s * opened[5], next_z(s) - s)
            rough = rough + limited(fore, back)
            volume = vol[x, j]
            root = jnp.exp(jnp.log(jnp.abs(volume)) * (1.0 / 3.0))
            root = jnp.where(volume < 0.0, -root, root)
            compress = jnp.maximum(-s, 0.0)
            quad = (root * root) * (0.0625 * compress) * (compress + rough)
            g, e = gamma[i, j], energy[i, j]
            base = (g - 1.0) * e
            both = base + quad
            ratio = root[:, :BZ] * lax.rsqrt(g[:, :BZ] * base[:, :BZ] + quad[:, :BZ])
            low = jnp.minimum(low, jnp.where(place.counted(i - 1, j), ratio, jnp.inf))
            work[i, j] = s * both
            t = jnp.where(place.present(i - 1, j), density[i, j] * inv[x, j] * both, 0.0)
            for d in range(3):
                t0, t1, t2 = t * cof[3 * d, x, j], t * cof[3 * d + 1, x, j], t * cof[3 * d + 2, x, j]
                for n, value in enumerate((t0 + t1, t0 - t1, t2)):
                    terms[3 * d + n, i, j + 1] = value
                    if j == GROUPS - 1:
                        terms[3 * d + n, i, 0] = prev_row(value)
        return low

    low = lax.fori_loop(0, EX, plane_step, jnp.full((8, BZ), jnp.inf, jnp.float32))
    low = jnp.broadcast_to(jnp.min(low, axis=0, keepdims=True), (8, BZ))
    for r in range(0, least.shape[0], 8):
        least[r : r + 8] = low


def force_of(terms, d, x, j):
    m, n, t = 3 * d, 3 * d + 1, 3 * d + 2
    r = terms[m, x, j] - terms[n, x + 1, j] + terms[n, x, j + 1] - terms[m, x + 1, j + 1]
    q = (terms[t, x, j] + terms[t, x + 1, j]) + (terms[t, x, j + 1] + terms[t, x + 1, j + 1])
    return (r - q) + prev_z(r + q)


def first_step(
    where, main, z_low, z_high,
    fs_d, fd_d, vel, energy, density, gamma, terms, work, least,
    fs, fd, cof, vol, inv, strain,
):
    place = Place(where)
    lane = lax.broadcasted_iota(jnp.int32, (8, BZ), 1)

    def extended(k, j):
        slot, q = divmod(k * GROUPS + j, 32)
        high = z_high[8 * slot : 8 * slot + 8]
        high = pltpu.roll(high, BZ - 4 * q, 1) if q else high
        low = z_low[8 * slot : 8 * slot + 8]
        low = pltpu.roll(low, BZ - 4 - 4 * q, 1) if q < 31 else low
        return jnp.concatenate([main[k, j], jnp.where(lane < BZ // 2, high, low)], axis=1)

    for k, field, plane in slab_ids():
        for j in range(GROUPS):
            value = extended(k, j)
            if field < 6:
                after = next_z(value)
                both, gap = value + after, after - value
                for out, v in ((fs, both), (fd, gap)):
                    out[field, plane, j] = v
                    if j == 0:
                        out[field, plane, GROUPS] = next_row(v)
                if field < 3:
                    fs_d[field, plane, j] = both
                    fd_d[field, plane, j] = gap
                else:
                    vel[field - 3, plane, j] = value
            else:
                (energy, density, gamma)[field - 6][plane, j] = value
    strain_pass(place, fs, fd, cof, vol, inv, strain)
    stress_pass(place, cof, vol, inv, strain, energy, density, gamma, terms, work, least)


def first_push(where, density, terms, accel_low, accel_mid, accel_high, unmass, held):
    place = Place(where)
    for i in range(EX):
        for j in range(GROUPS):
            value = jnp.where(place.present(i - 1, j), density[i, j], 0.0)
            held[i, j + 1] = value
            if j == GROUPS - 1:
                held[i, 0] = prev_row(value)
    for x in range(BX):
        for j in range(GROUPS):
            mass = (held[x, j] + held[x + 1, j]) + (held[x, j + 1] + held[x + 1, j + 1])
            mass = 0.125 * (mass + prev_z(mass))
            some = mass > 0.0
            recip = jnp.where(some, 1.0 / jnp.where(some, mass, 1.0), 0.0)
            unmass[x, j] = recip[:, :BZ]
            for d in range(3):
                value = force_of(terms, d, x, j) * recip
                if x < 2:
                    accel_low[d, x, j] = value
                elif x < BX - 2:
                    accel_mid[d, x - 2, j] = value
                else:
                    accel_high[d, x - BX + 2, j] = value


def least_of(ref):
    return jnp.min(ref[...])


def second_step(
    where, lows, fs_d, fd_d, vel, energy, density, gamma, work,
    got_low, accel_low, accel_mid, accel_high, got_high,
    new_vel, new_energy, terms, new_work, least,
    fs, fd, cof, vol, inv, strain, moved,
):
    place = Place(where)
    dt = least_of(lows) * 0.0625
    wall = [jnp.where(place.flag[2 * d] == 1, 0, -FAR) for d in range(3)]
    last = (place.nx - 1, place.ny - 1, place.nz - 1)
    edge = [jnp.where(place.flag[2 * d + 1] == 1, last[d], -FAR) for d in range(3)]
    on_z = (place.col == wall[2]) | (place.col == edge[2])
    for x in range(PX):
        gx = place.x0 + x - 2
        on_x = (gx == wall[0]) | (gx == edge[0])
        for j in range(GROUPS):
            for d in range(3):
                if x < 2:
                    push = got_low[d, x, j]
                elif x < 4:
                    push = accel_low[d, x - 2, j]
                elif x < BX:
                    push = accel_mid[d, x - 4, j]
                elif x < BX + 2:
                    push = accel_high[d, x - BX, j]
                else:
                    push = got_high[d, x - BX - 2, j]
                v = vel[d, x, j] + dt * push
                if d == 0:
                    v = jnp.where(on_x, 0.0, v)
                elif d == 1:
                    v = jnp.where((place.row == wall[1] - j) | (place.row == edge[1] - j), 0.0, v)
                else:
                    v = jnp.where(on_z, 0.0, v)
                if 2 <= x < BX + 2:
                    new_vel[d, x - 2, j] = v[:, :BZ]
                after = next_z(v)
                both, gap = v + after, after - v
                for out, old, u in ((fs, fs_d, both), (fd, fd_d, gap)):
                    w = old[d, x, j] + dt * u
                    out[d, x, j] = w
                    out[d + 3, x, j] = u
                    if j == 0:
                        out[d, x, GROUPS] = next_row(w)
                        out[d + 3, x, GROUPS] = next_row(u)
    for i in range(EX):
        for j in range(GROUPS):
            e = energy[i, j]
            e = jnp.where(place.present(i - 1, j), e - dt * work[i, j], e)
            moved[i, j] = e
            if i:
                new_energy[i - 1, j] = e[:, :BZ]
    strain_pass(place, fs, fd, cof, vol, inv, strain)
    stress_pass(place, cof, vol, inv, strain, moved, density, gamma, terms, new_work, least)


def second_push(
    terms, unmass, new_vel, new_energy, new_work,
    out_accel, out_vel, out_energy, out_work, stage,
):
    for x in range(BX):
        for j in range(GROUPS):
            rows = pl.ds(j, 8, stride=GROUPS)
            for d in range(3):
                stage[x, d, rows, :] = force_of(terms, d, x, j)[:, :BZ] * unmass[x, j]
                stage[x, 3 + d, rows, :] = new_vel[d, x, j]
            stage[x, 6, rows, :] = new_energy[x, j]
            stage[x, 7, rows, :] = new_work[x + 1, j, :, :BZ]
        for d in range(3):
            out_accel[d, x] = stage[x, d, 4 : BY + 4, :]
            out_vel[d, x] = stage[x, 3 + d, 4 : BY + 4, :]
        out_energy[x] = stage[x, 6, 4 : BY + 4, :]
        out_work[x] = stage[x, 7, 4 : BY + 4, :]


def finish(where, lows, again, disp, vel, accel, energy, work, new_disp, new_vel, new_energy):
    dt = least_of(lows) * 0.0625
    dt2 = least_of(again) * 0.0625
    x0, y0, z0 = where[0], where[1], where[2]
    nx, ny, nz = where[3], where[4], where[5]
    row = lax.broadcasted_iota(jnp.int32, (BY, BZ), 0) + y0
    col = lax.broadcasted_iota(jnp.int32, (BY, BZ), 1) + z0

    def walled(at, low, high, count):
        return ((at == 0) & (where[low] == 1)) | ((at == count - 1) & (where[high] == 1))

    on_y, on_z = walled(row, 8, 9, ny), walled(col, 10, 11, nz)
    inside = (row < ny - 1) & (col < nz - 1)
    for x in range(BX):
        on_x = walled(x0 + x, 6, 7, nx)
        for d in range(3):
            v = vel[d, x]
            u = jnp.where((on_x, on_y, on_z)[d], 0.0, v + dt2 * accel[d, x])
            new_vel[d, x] = u
            new_disp[d, x] = (disp[d, x] + dt * v) + dt2 * u
        e = energy[x]
        moved = jnp.where(inside, e - dt2 * work[x], e)
        new_energy[x] = jnp.where(x0 + x < nx - 1, moved, e)


def call(kernel, outs, args, smem=0, scratch=(), limit=48):
    specs = [
        pl.BlockSpec(memory_space=pltpu.SMEM if i < smem else pltpu.VMEM) for i in range(len(args))
    ]
    return pl.pallas_call(
        kernel,
        out_shape=[jax.ShapeDtypeStruct(s, jnp.float32) for s in outs],
        in_specs=specs,
        out_specs=[pl.BlockSpec(memory_space=pltpu.VMEM) for _ in outs],
        scratch_shapes=[pltpu.VMEM(s, jnp.float32) for s in scratch],
        compiler_params=pltpu.CompilerParams(vmem_limit_bytes=limit * MIB),
        name=kernel.__name__,
    )(*args)


def swap(up, down, axis):
    size = lax.axis_size(axis)
    ring = [(i, (i + 1) % size) for i in range(size)]
    low = lax.ppermute(up, axis, ring)
    high = lax.ppermute(down, axis, [(b, a) for a, b in ring])
    return low, high


def body(displacement, velocity, energy, density, region, adiabatic, face_flags):
    assert energy.shape == (BX, BY, BZ)
    sizes = (lax.axis_size("gx"), lax.axis_size(GY), lax.axis_size("gz"))
    devices = sizes[0] * sizes[1] * sizes[2]
    where = jnp.stack(
        [
            lax.axis_index("gx") * BX,
            lax.axis_index(GY) * BY,
            lax.axis_index("gz") * BZ,
            jnp.int32(sizes[0] * BX),
            jnp.int32(sizes[1] * BY),
            jnp.int32(sizes[2] * BZ),
        ]
    )
    where = jnp.concatenate([where, face_flags])
    block = (BX, BY, BZ)
    up, down, gamma = call(
        pack_x,
        [(15, BY, BZ), (12, BY, BZ), block],
        (adiabatic, displacement, velocity, energy, density, region),
        smem=1,
        limit=8,
    )
    x_low, x_high = swap(up, down, "gx")
    own = (displacement, velocity, energy, density, gamma, x_low, x_high)
    up, down = call(pack_y, [(4 * SLABS, BZ)] * 2, own, limit=8)
    y_low, y_high = swap(up, down, GY)
    main, up, down = call(
        pack_z,
        [(SLABS, GROUPS, 8, BZ), (8 * PACKED, BZ), (8 * PACKED, BZ)],
        (*own, y_low, y_high),
        scratch=[(SLABS, ROWS, BZ)],
        limit=16,
    )
    z_low, z_high = swap(up, down, "gz")

    chunk = (GROUPS, 8, LANES)
    slots = (GROUPS + 1, 8, LANES)
    passes = [
        (6, PX, *slots),
        (6, PX, *slots),
        (9, PX - 1, *chunk),
        (PX - 1, *chunk),
        (PX - 1, *chunk),
        (PX - 1, GROUPS + 2, 8, LANES),
    ]
    fs_d, fd_d, vel, e, rho, g, terms, work, least = call(
        first_step,
        [(3, PX, *chunk)] * 3 + [(EX, *chunk)] * 3 + [(9, EX, *slots), (EX, *chunk), (devices, BZ)],
        (where, main, z_low, z_high),
        smem=1,
        scratch=passes,
        limit=36,
    )
    lows = lax.all_to_all(least, AXES, 0, 0, tiled=True)
    a_low, a_mid, a_high, unmass = call(
        first_push,
        [(3, 2, *chunk), (3, BX - 4, *chunk), (3, 2, *chunk), (BX, GROUPS, 8, BZ)],
        (where, rho, terms),
        smem=1,
        scratch=[(EX, *slots)],
        limit=16,
    )
    got_low, got_high = swap(a_high, a_low, "gx")
    new_vel, new_e, terms, work, least = call(
        second_step,
        [(3, BX, GROUPS, 8, BZ), (BX, GROUPS, 8, BZ), (9, EX, *slots), (EX, *chunk), (devices, BZ)],
        (where, lows, fs_d, fd_d, vel, e, rho, g, work, got_low, a_low, a_mid, a_high, got_high),
        smem=1,
        scratch=[*passes, (EX, *chunk)],
        limit=36,
    )
    again = lax.all_to_all(least, AXES, 0, 0, tiled=True)
    accel, vel, e, work = call(
        second_push,
        [(3, *block), (3, *block), block, block],
        (terms, unmass, new_vel, new_e, work),
        scratch=[(BX, 8, ROWS, BZ)],
        limit=16,
    )
    return tuple(
        call(
            finish,
            [(3, *block), (3, *block), block],
            (where, lows, again, displacement, vel, accel, e, work),
            smem=1,
            limit=12,
        )
    )


def solution(mesh):
    torus = Mesh(
        mesh.devices.reshape(mesh.shape["gx"], mesh.shape["gy"] // 2, 2, mesh.shape["gz"]), AXES
    )
    nodes, elements = P(None, "gx", GY, "gz"), P("gx", GY, "gz")
    return jax.shard_map(
        body,
        mesh=torus,
        in_specs=(nodes, nodes, elements, elements, elements, P(), P()),
        out_specs=(nodes, nodes, elements),
        check_vma=False,
    )
```

```python
import functools

import jax
import jax.numpy as jnp
from jax import lax
from jax.experimental import pallas as pl
from jax.experimental.pallas import tpu as pltpu
from jax.sharding import Mesh
from jax.sharding import PartitionSpec as P

GY = ("gy_0", "gy_1")
AXES = ("gx", "gy_0", "gy_1", "gz")

BX, BY, BZ = 8, 32, 128
PX = BX + 4
EX = BX + 1
ROWS = BY + 8
GROUPS = ROWS // 8
LANES = 2 * BZ
SLABS = 6 * PX + 3 * EX
PAIRS = -(-EX // 2)
PACKED = PX + PAIRS
FAR = 1 << 20
ENERGY, DENSITY, GAMMA, WORK = range(4)
MIB = 1 << 20


def next_z(v):
    return pltpu.roll(v, LANES - 1, 1)


def prev_z(v):
    return pltpu.roll(v, 1, 1)


def next_row(v):
    return pltpu.roll(v, 7, 0)


def prev_row(v):
    return pltpu.roll(v, 1, 0)


def slab_ids():
    for field in range(6):
        for plane in range(PX):
            yield field * PX + plane, field, plane
    for field in range(6, 9):
        for plane in range(EX):
            yield 6 * PX + (field - 6) * EX + plane, field, plane


def pack_x(
    gamma_table, disp, vel, energy, density, region,
    up, down, gamma, disp_in, vel_in, energy_in, density_in,
    ids, sems,
):
    moves = ((region, ids), (disp, disp_in), (vel, vel_in), (energy, energy_in), (density, density_in))
    copies = [pltpu.make_async_copy(a, b, sems.at[i]) for i, (a, b) in enumerate(moves)]
    for c in copies:
        c.start()
    copies[0].wait()
    kinds = ids[...]
    value = jnp.zeros(kinds.shape, jnp.float32)
    for r in range(gamma_table.shape[0]):
        value = jnp.where(kinds == r, gamma_table[r], value)
    gamma[...] = value
    up[14] = value[BX - 1]
    for c in copies[1:]:
        c.wait()
    for field in range(6):
        src = disp_in if field < 3 else vel_in
        for p in range(2):
            up[2 * field + p] = src[field % 3, BX - 2 + p]
            down[2 * field + p] = src[field % 3, p]
    up[12] = energy_in[BX - 1]
    up[13] = density_in[BX - 1]


def slab_source(field, plane, disp, vel, energy, density, gamma, x_low, x_high):
    if field < 6:
        if plane < 2:
            return x_low, (2 * field + plane,)
        if plane < BX + 2:
            return (disp if field < 3 else vel), (field % 3, plane - 2)
        return x_high, (2 * field + plane - BX - 2,)
    if plane == 0:
        return x_low, (12 + field - 6,)
    return (energy, density, gamma)[field - 6], (plane - 1,)


def pack_y(disp, vel, energy, density, gamma, x_low, x_high, up, down):
    for k, field, plane in slab_ids():
        ref, at = slab_source(field, plane, disp, vel, energy, density, gamma, x_low, x_high)
        up[4 * k : 4 * k + 4] = ref[(*at, slice(BY - 4, BY))]
        down[4 * k : 4 * k + 4] = ref[(*at, slice(0, 4))]


def pack_z(disp, vel, energy, density, gamma, x_low, x_high, y_low, y_high, main, up, down, stage):
    quad = lax.broadcasted_iota(jnp.int32, (8, BZ), 1) // 4
    for k, field, plane in slab_ids():
        ref, at = slab_source(field, plane, disp, vel, energy, density, gamma, x_low, x_high)
        stage[k, 0:4] = y_low[4 * k : 4 * k + 4]
        stage[k, 4 : BY + 4] = ref[(*at, slice(0, BY))]
        stage[k, BY + 4 : BY + 8] = y_high[4 * k : 4 * k + 4]

    def pack(parts, slot):
        to_up = jnp.zeros((8, BZ), jnp.float32)
        to_down = jnp.zeros((8, BZ), jnp.float32)
        for q, k, j in parts:
            value = stage[k, pl.ds(j, 8, stride=GROUPS), :]
            main[k, j] = value
            to_up = jnp.where(quad == q, pltpu.roll(value, (4 * q + 4) % BZ, 1), to_up)
            here = pltpu.roll(value, 4 * q, 1) if q else value
            to_down = jnp.where(quad == q, here, to_down)
        up[slot] = to_up
        down[slot] = to_down

    def node_plane(plane, carry):
        pack([(f * GROUPS + j, f * PX + plane, j) for f in range(6) for j in range(GROUPS)], plane)
        return carry

    def element_planes(pair, carry, count=2):
        pack(
            [
                ((h * 3 + f) * GROUPS + j, 6 * PX + f * EX + 2 * pair + h, j)
                for h in range(count)
                for f in range(3)
                for j in range(GROUPS)
            ],
            PX + pair,
        )
        return carry

    lax.fori_loop(0, PX, node_plane, 0)
    lax.fori_loop(0, EX // 2, element_planes, 0)
    if EX % 2:
        element_planes(EX // 2, 0, 1)


class Place:
    def __init__(self, where):
        self.x0, self.y0, self.z0 = where[0], where[1], where[2]
        self.nx, self.ny, self.nz = where[3], where[4], where[5]
        self.flag = [where[6 + i] for i in range(6)]
        sublane = lax.broadcasted_iota(jnp.int32, (8, LANES), 0)
        lane = lax.broadcasted_iota(jnp.int32, (8, LANES), 1)
        self.row = GROUPS * sublane + (self.y0 - 4)
        self.col = jnp.where(lane < LANES - BZ // 2, lane, lane - LANES) + self.z0
        inside = (self.col >= 0) & (self.col < self.nz - 1)
        self.row_inside = jnp.where(inside, self.row, -FAR)

    def present(self, plane, j):
        x = self.x0 + plane
        ok = (x >= 0) & (x < self.nx - 1)
        top = jnp.where(ok, self.ny - 1 - j, -2 * FAR)
        return (self.row_inside >= -j) & (self.row_inside < top)

    def counted(self, plane, j):
        x = self.x0 + plane
        ok = (x >= 0) & (x < self.nx - 1)
        top = jnp.where(ok, jnp.minimum(self.ny - 1, self.y0 + BY) - j, -2 * FAR)
        rows = self.row_inside[:, :BZ]
        return (rows >= self.y0 - j) & (rows < top)


def open_factor(flag):
    return jnp.where(flag == 1, 0.0, 1.0)


def strain_pass(fs_d, fd_d, fs_v, fd_v, cof, vol, inv, strain):
    def plane_step(x, carry):
        for j in range(GROUPS):
            grad = []
            for n in range(6):
                f = n % 3
                fs, fd = (fs_d, fd_d) if n < 3 else (fs_v, fd_v)
                a, b = fs[f, x, j], fs[f, x + 1, j]
                c, d = fs[f, x, j + 1], fs[f, x + 1, j + 1]
                p, q = d - a, b - c
                gz = (fd[f, x, j] + fd[f, x + 1, j]) + (fd[f, x, j + 1] + fd[f, x + 1, j + 1])
                grad.append([p + q, p - q, gz])
            m = [[grad[d][e] + 4.0 if d == e else grad[d][e] for e in range(3)] for d in range(3)]
            g = grad[3:]

            def minor(r, s, u, w):
                return m[r][u] * m[s][w] - m[r][w] * m[s][u]

            c = [
                [minor(1, 2, 1, 2), minor(1, 2, 2, 0), minor(1, 2, 0, 1)],
                [minor(2, 0, 1, 2), minor(2, 0, 2, 0), minor(2, 0, 0, 1)],
                [minor(0, 1, 1, 2), minor(0, 1, 2, 0), minor(0, 1, 0, 1)],
            ]
            volume = m[0][0] * c[0][0] + m[0][1] * c[0][1] + m[0][2] * c[0][2]
            change = c[0][0] * g[0][0]
            for d in range(3):
                for e in range(3):
                    if d or e:
                        change = change + c[d][e] * g[d][e]
                    cof[3 * d + e, x, j] = c[d][e]
            inverse = 1.0 / volume
            rate = change * inverse
            vol[x, j] = volume
            inv[x, j] = inverse
            strain[x, j + 1] = rate
            if j == 0:
                strain[x, GROUPS + 1] = next_row(rate)
            if j == GROUPS - 1:
                strain[x, 0] = prev_row(rate)
        return carry

    lax.fori_loop(0, PX - 1, plane_step, 0)


def limited(forward, backward):
    return jnp.maximum(jnp.minimum(forward, backward), 0.0) - jnp.minimum(
        jnp.maximum(forward, backward), 0.0
    )


def stress_pass(place, cof, vol, inv, strain, elems, terms, least, plane_done=None):
    opened = [open_factor(f) for f in place.flag]

    def plane_step(i, low):
        x = i + 1
        gx = place.x0 + i - 1
        for j in range(GROUPS):
            s = strain[x, j + 1]
            back = jnp.where(gx == 0, s * opened[0], s - strain[x - 1, j + 1])
            fore = jnp.where(gx == place.nx - 2, -s * opened[1], strain[x + 1, j + 1] - s)
            rough = limited(fore, back)
            back = jnp.where(place.row == -j, s * opened[2], s - strain[x, j])
            fore = jnp.where(
                place.row == place.ny - 2 - j, -s * opened[3], strain[x, j + 2] - s
            )
            rough = rough + limited(fore, back)
            back = jnp.where(place.col == 0, s * opened[4], s - prev_z(s))
            fore = jnp.where(place.col == place.nz - 2, -s * opened[5], next_z(s) - s)
            rough = rough + limited(fore, back)
            volume = vol[x, j]
            root = jnp.exp(jnp.log(jnp.abs(volume)) * (1.0 / 3.0))
            root = jnp.where(volume < 0.0, -root, root)
            compress = jnp.maximum(-s, 0.0)
            quad = (root * root) * (0.0625 * compress) * (compress + rough)
            g, e = elems[i, GAMMA, j], elems[i, ENERGY, j]
            base = (g - 1.0) * e
            both = base + quad
            ratio = root[:, :BZ] * lax.rsqrt(g[:, :BZ] * base[:, :BZ] + quad[:, :BZ])
            low = jnp.minimum(low, jnp.where(place.counted(i - 1, j), ratio, jnp.inf))
            elems[i, WORK, j] = s * both
            t = elems[i, DENSITY, j] * inv[x, j] * both
            t = jnp.where(place.present(i - 1, j), t, 0.0)
            for d in range(3):
                t0, t1, t2 = t * cof[3 * d, x, j], t * cof[3 * d + 1, x, j], t * cof[3 * d + 2, x, j]
                for n, value in enumerate((t0 + t1, t0 - t1, t2)):
                    terms[3 * d + n, i, j + 1] = value
                    if j == GROUPS - 1:
                        terms[3 * d + n, i, 0] = prev_row(value)
        if plane_done:
            plane_done(i)
        return low

    low = lax.fori_loop(0, EX, plane_step, jnp.full((8, BZ), jnp.inf, jnp.float32))
    low = jnp.broadcast_to(jnp.min(low, axis=0, keepdims=True), (8, BZ))
    for r in range(0, least.shape[0], 8):
        least[r : r + 8] = low


def force_of(terms, d, x, j):
    m, n, t = 3 * d, 3 * d + 1, 3 * d + 2
    r = terms[m, x, j] - terms[n, x + 1, j] + terms[n, x, j + 1] - terms[m, x + 1, j + 1]
    q = (terms[t, x, j] + terms[t, x + 1, j]) + (terms[t, x, j + 1] + terms[t, x + 1, j + 1])
    return (r - q) + prev_z(r + q)


def store_sums(sums, gaps, field, plane, j, both, gap):
    for out, v in ((sums, both), (gaps, gap)):
        out[field, plane, j] = v
        if j == 0:
            out[field, plane, GROUPS] = next_row(v)


def first_step(
    where, main, z_low, z_high,
    nodes_out, elems_out, accel_low, accel_mid, accel_high, unmass_out, least_out,
    fs_d, fd_d, fs_v, fd_v, cof, vol, inv, strain, terms,
    nodes, elems, accel, unmass, least, held, node_sems, elem_sems, sems,
):
    place = Place(where)
    lane = lax.broadcasted_iota(jnp.int32, (8, BZ), 1)

    def extended(k, j, slot, q):
        high, low = z_high[slot], z_low[slot]
        high = pltpu.roll(high, BZ - 4 * q, 1) if q else high
        low = pltpu.roll(low, BZ - 4 - 4 * q, 1) if q < 31 else low
        return jnp.concatenate([main[k, j], jnp.where(lane < BZ // 2, high, low)], axis=1)

    def nodes_copy(plane):
        return pltpu.make_async_copy(nodes.at[plane], nodes_out.at[plane], node_sems.at[plane])

    def elems_copy(i):
        return pltpu.make_async_copy(elems.at[i], elems_out.at[i], elem_sems.at[i])

    def node_plane(plane, carry):
        for field in range(6):
            for j in range(GROUPS):
                value = extended(field * PX + plane, j, plane, field * GROUPS + j)
                nodes[plane, field, j] = value
                after = next_z(value)
                sums, gaps = (fs_d, fd_d) if field < 3 else (fs_v, fd_v)
                store_sums(sums, gaps, field % 3, plane, j, value + after, after - value)
        nodes_copy(plane).start()
        return carry

    def element_planes(pair, carry, count=2):
        for h in range(count):
            for f in range(3):
                for j in range(GROUPS):
                    k = 6 * PX + f * EX + 2 * pair + h
                    value = extended(k, j, PX + pair, (h * 3 + f) * GROUPS + j)
                    elems[2 * pair + h, f, j] = value
        return carry

    lax.fori_loop(0, PX, node_plane, 0)
    lax.fori_loop(0, EX // 2, element_planes, 0)
    if EX % 2:
        element_planes(EX // 2, 0, 1)
    strain_pass(fs_d, fd_d, fs_v, fd_v, cof, vol, inv, strain)
    stress_pass(
        place, cof, vol, inv, strain, elems, terms, least, lambda i: elems_copy(i).start()
    )
    least_copy = pltpu.make_async_copy(least, least_out, sems.at[0])
    least_copy.start()
    copies = [least_copy]
    for i in range(EX):
        for j in range(GROUPS):
            value = jnp.where(place.present(i - 1, j), elems[i, DENSITY, j], 0.0)
            held[i, j + 1] = value
            if j == GROUPS - 1:
                held[i, 0] = prev_row(value)

    def push_plane(x, carry=0):
        for j in range(GROUPS):
            mass = (held[x, j] + held[x + 1, j]) + (held[x, j + 1] + held[x + 1, j + 1])
            mass = 0.125 * (mass + prev_z(mass))
            some = mass > 0.0
            recip = jnp.where(some, 1.0 / jnp.where(some, mass, 1.0), 0.0)
            unmass[x, j] = recip[:, :BZ]
            for d in range(3):
                accel[x, d, j] = force_of(terms, d, x, j) * recip
        return carry

    def send(source, target, n):
        copies.append(pltpu.make_async_copy(source, target, sems.at[n]))
        copies[-1].start()

    lax.fori_loop(0, 2, push_plane, 0)
    send(accel.at[0:2], accel_low, 1)
    lax.fori_loop(BX - 2, BX, push_plane, 0)
    send(accel.at[BX - 2 : BX], accel_high, 2)
    lax.fori_loop(2, BX - 2, push_plane, 0)
    send(accel.at[2 : BX - 2], accel_mid, 3)
    send(unmass, unmass_out, 4)
    for plane in range(PX):
        nodes_copy(plane).wait()
    for i in range(EX):
        elems_copy(i).wait()
    for c in copies:
        c.wait()


def least_of(ref):
    return jnp.min(ref[...])


def second_step(
    where, lows,
    nodes_in, elems_in, unmass_in, got_low, accel_low, accel_mid, accel_high, got_high,
    natural_out, least_out,
    fs_d, fd_d, fs_v, fd_v, cof, vol, inv, strain, terms,
    nodes, elems, accel, unmass, new_vel, natural, stage, least,
    node_sems, accel_sems, plane_sems, sems,
):
    def nodes_copy(x):
        return pltpu.make_async_copy(nodes_in.at[x], nodes.at[x], node_sems.at[x])

    parts, at = [], 0
    for n, source in enumerate((got_low, accel_low, accel_mid, accel_high, got_high)):
        count = source.shape[0]
        copy = pltpu.make_async_copy(source, accel.at[at : at + count], accel_sems.at[n])
        parts.append((at, count, copy))
        at += count
    for first, count, copy in parts:
        copy.start()
        for x in range(first, first + count):
            nodes_copy(x).start()
    elems_copy = pltpu.make_async_copy(elems_in, elems, sems.at[1])
    unmass_copy = pltpu.make_async_copy(unmass_in, unmass, sems.at[2])
    elems_copy.start()
    unmass_copy.start()
    place = Place(where)
    dt = least_of(lows) * 0.0625
    wall = [jnp.where(place.flag[2 * d] == 1, 0, -FAR) for d in range(3)]
    last = (place.nx - 1, place.ny - 1, place.nz - 1)
    edge = [jnp.where(place.flag[2 * d + 1] == 1, last[d], -FAR) for d in range(3)]
    on_z = (place.col == wall[2]) | (place.col == edge[2])

    def move_plane(x, carry):
        nodes_copy(x).wait()
        gx = place.x0 + x - 2
        on_x = (gx == wall[0]) | (gx == edge[0])
        for j in range(GROUPS):
            for d in range(3):
                v = nodes[x, d + 3, j] + dt * accel[x, d, j]
                if d == 0:
                    v = jnp.where(on_x, 0.0, v)
                elif d == 1:
                    v = jnp.where((place.row == wall[1] - j) | (place.row == edge[1] - j), 0.0, v)
                else:
                    v = jnp.where(on_z, 0.0, v)
                new_vel[x, d, j] = v[:, :BZ]
                after = next_z(v)
                store_sums(fs_v, fd_v, d, x, j, v + after, after - v)
                v = nodes[x, d, j] + dt * v
                after = next_z(v)
                store_sums(fs_d, fd_d, d, x, j, v + after, after - v)

        return carry

    for first, count, copy in parts:
        copy.wait()
        lax.fori_loop(first, first + count, move_plane, 0)
    elems_copy.wait()

    def heat_plane(i, carry):
        for j in range(GROUPS):
            e = elems[i, ENERGY, j]
            moved = e - dt * elems[i, WORK, j]
            elems[i, ENERGY, j] = jnp.where(place.present(i - 1, j), moved, e)
        return carry

    lax.fori_loop(0, EX, heat_plane, 0)
    unmass_copy.wait()
    strain_pass(fs_d, fd_d, fs_v, fd_v, cof, vol, inv, strain)
    stress_pass(place, cof, vol, inv, strain, elems, terms, least)
    least_copy = pltpu.make_async_copy(least, least_out, sems.at[0])
    least_copy.start()

    def natural_copy(x):
        return pltpu.make_async_copy(natural.at[x], natural_out.at[x], plane_sems.at[x])

    def push_plane(x, carry):
        for j in range(GROUPS):
            rows = pl.ds(j, 8, stride=GROUPS)
            for d in range(3):
                stage[x, d, rows, :] = force_of(terms, d, x, j)[:, :BZ] * unmass[x, j]
                stage[x, 3 + d, rows, :] = new_vel[x + 2, d, j]
            stage[x, 6, rows, :] = elems[x + 1, ENERGY, j, :, :BZ]
            stage[x, 7, rows, :] = elems[x + 1, WORK, j, :, :BZ]
        for n in range(8):
            natural[x, n] = stage[x, n, 4 : BY + 4, :]
        natural_copy(x).start()
        return carry

    lax.fori_loop(0, BX, push_plane, 0)
    for x in range(BX):
        natural_copy(x).wait()
    least_copy.wait()


def finish(where, lows, again, disp, natural, new_disp, new_vel, new_energy):
    dt = least_of(lows) * 0.0625
    dt2 = least_of(again) * 0.0625
    x0, y0, z0 = where[0], where[1], where[2]
    nx, ny, nz = where[3], where[4], where[5]
    row = lax.broadcasted_iota(jnp.int32, (BY, BZ), 0) + y0
    col = lax.broadcasted_iota(jnp.int32, (BY, BZ), 1) + z0

    def walled(at, low, high, count):
        return ((at == 0) & (where[low] == 1)) | ((at == count - 1) & (where[high] == 1))

    on_y, on_z = walled(row, 8, 9, ny), walled(col, 10, 11, nz)
    inside = (row < ny - 1) & (col < nz - 1)
    for x in range(BX):
        on_x = walled(x0 + x, 6, 7, nx)
        for d in range(3):
            v = natural[x, 3 + d]
            u = jnp.where((on_x, on_y, on_z)[d], 0.0, v + dt2 * natural[x, d])
            new_vel[d, x] = u
            new_disp[d, x] = (disp[d, x] + dt * v) + dt2 * u
        e = natural[x, 6]
        moved = jnp.where(inside, e - dt2 * natural[x, 7], e)
        new_energy[x] = jnp.where(x0 + x < nx - 1, moved, e)


def call(
    kernel, outs, args, smem=0, near=0, scratch=(), limit=48, space=pltpu.VMEM, out_space=pltpu.VMEM
):
    spaces = [pltpu.SMEM] * smem + [pltpu.VMEM] * near
    spaces += [space] * (len(args) - len(spaces))
    specs = [pl.BlockSpec(memory_space=m) for m in spaces]
    pinned = [
        pltpu.with_memory_space_constraint(a, m) if m is pltpu.HBM else a
        for a, m in zip(args, spaces, strict=True)
    ]
    shape = pltpu.HBM if out_space is pltpu.HBM else jax.ShapeDtypeStruct
    return pl.pallas_call(
        kernel,
        out_shape=[shape(s, jnp.float32) for s in outs],
        in_specs=specs,
        out_specs=[pl.BlockSpec(memory_space=out_space) for _ in outs],
        scratch_shapes=[pltpu.VMEM(s, jnp.float32) if isinstance(s, tuple) else s for s in scratch],
        compiler_params=pltpu.CompilerParams(vmem_limit_bytes=limit * MIB),
        name=kernel.__name__,
    )(*pinned)


def swap(up, down, axis):
    size = lax.axis_size(axis)
    ring = [(i, (i + 1) % size) for i in range(size)]
    low = lax.ppermute(up, axis, ring)
    high = lax.ppermute(down, axis, [(b, a) for a, b in ring])
    return low, high


def body(displacement, velocity, energy, density, region, adiabatic, face_flags):
    assert energy.shape == (BX, BY, BZ)
    sizes = (lax.axis_size("gx"), lax.axis_size(GY), lax.axis_size("gz"))
    devices = sizes[0] * sizes[1] * sizes[2]
    where = jnp.stack(
        [
            lax.axis_index("gx") * BX,
            lax.axis_index(GY) * BY,
            lax.axis_index("gz") * BZ,
            jnp.int32(sizes[0] * BX),
            jnp.int32(sizes[1] * BY),
            jnp.int32(sizes[2] * BZ),
        ]
    )
    where = jnp.concatenate([where, face_flags])
    block = (BX, BY, BZ)
    up, down, *own = call(
        pack_x,
        [(15, BY, BZ), (12, BY, BZ), block, (3, *block), (3, *block), block, block],
        (adiabatic, displacement, velocity, energy, density, region),
        smem=1,
        scratch=[pltpu.VMEM(block, jnp.int32), pltpu.SemaphoreType.DMA((5,))],
        limit=2,
        space=pltpu.HBM,
    )
    gamma, *own = own
    x_low, x_high = swap(up, down, "gx")
    own = (*own, gamma, x_low, x_high)
    up, down = call(pack_y, [(4 * SLABS, BZ)] * 2, own, limit=2)
    y_low, y_high = swap(up, down, GY)
    main, up, down = call(
        pack_z,
        [(SLABS, GROUPS, 8, BZ), (PACKED, 8, BZ), (PACKED, 8, BZ)],
        (*own, y_low, y_high),
        scratch=[(SLABS, ROWS, BZ)],
        limit=4,
    )
    z_low, z_high = swap(up, down, "gz")

    chunk = (GROUPS, 8, LANES)
    half = (GROUPS, 8, BZ)
    slots = (GROUPS + 1, 8, LANES)
    passes = [(3, PX, *slots)] * 4 + [
        (9, PX - 1, *chunk),
        (PX - 1, *chunk),
        (PX - 1, *chunk),
        (PX - 1, GROUPS + 2, 8, LANES),
        (9, EX, *slots),
    ]
    sem = pltpu.SemaphoreType.DMA
    nodes, elems, a_low, a_mid, a_high, unmass, least = call(
        first_step,
        [
            (PX, 6, *chunk),
            (EX, 4, *chunk),
            (2, 3, *chunk),
            (BX - 4, 3, *chunk),
            (2, 3, *chunk),
            (BX, *half),
            (devices, BZ),
        ],
        (where, main, z_low, z_high),
        smem=1,
        scratch=[
            *passes,
            (PX, 6, *chunk),
            (EX, 4, *chunk),
            (BX, 3, *chunk),
            (BX, *half),
            (devices, BZ),
            (EX, *slots),
            sem((PX,)),
            sem((EX,)),
            sem((5,)),
        ],
        limit=28,
        out_space=pltpu.HBM,
    )
    lows = lax.all_to_all(least, AXES, 0, 0, tiled=True)
    got_low, got_high = swap(a_high, a_low, "gx")
    natural, least = call(
        second_step,
        [(BX, 8, BY, BZ), (devices, BZ)],
        (where, lows, nodes, elems, unmass, got_low, a_low, a_mid, a_high, got_high),
        smem=1,
        near=1,
        scratch=[
            *passes,
            (PX, 6, *chunk),
            (EX, 4, *chunk),
            (PX, 3, *chunk),
            (BX, *half),
            (PX, 3, *half),
            (BX, 8, BY, BZ),
            (BX, 8, ROWS, BZ),
            (devices, BZ),
            sem((PX,)),
            sem((5,)),
            sem((BX,)),
            sem((3,)),
        ],
        limit=32,
        space=pltpu.HBM,
        out_space=pltpu.HBM,
    )
    again = lax.all_to_all(least, AXES, 0, 0, tiled=True)
    return tuple(
        call(
            finish,
            [(3, *block), (3, *block), block],
            (where, lows, again, displacement, natural),
            smem=1,
            limit=4,
        )
    )


def solution(mesh):
    torus = Mesh(
        mesh.devices.reshape(mesh.shape["gx"], mesh.shape["gy"] // 2, 2, mesh.shape["gz"]), AXES
    )
    nodes, elements = P(None, "gx", GY, "gz"), P("gx", GY, "gz")
    return jax.shard_map(
        body,
        mesh=torus,
        in_specs=(nodes, nodes, elements, elements, elements, P(), P()),
        out_specs=(nodes, nodes, elements),
        check_vma=False,
    )
```
